256 devices in a mesh: section: 16 (over y, z_lo, core), tp: 16 (over z_hi, x).
Axes of the slice: x: 4, y: 4, z: 8 (z_hi: 4, z_lo: 2; z = z_hi * 2 + z_lo), core: 2. Of those that a mesh axis runs over, the one named last changes fastest.
Arguments:
- embedded: bfloat16 [768, 4096], P('tp'), may hold values from -20 to 20
- previous_out: bfloat16 [16, 768, 4096], P('section', 'tp'), may hold values from -20 to 20
- top_grad: bfloat16 [768, 4096], P('tp'), may hold values from -6 to 6
- grad_out: bfloat16 [16, 768, 4096], P('section', 'tp'), may hold values from -6 to 6
- saved_input: bfloat16 [16, 768, 4096], P('section', 'tp'), may hold values from -20 to 20
- saved_qkv: bfloat16 [16, 768, 3, 2048], P('section', None, None, 'tp'), may hold values from -64 to 64
- norm_gain: float32 [16, 2, 4096], P('section'), may hold values from 0.1 to 1.9
- qkv_weight: bfloat16 [16, 2, 4096, 3, 2048], P('section', None, None, None, 'tp'), may hold values from -4 to 4
- out_weight: bfloat16 [16, 2, 2048, 4096], P('section', None, 'tp'), may hold values from -0.125 to 0.125
- modality: int32 [16, 2, 768], P('section'), may hold values from 0 to 1, as said below
- documents: int32 [16, 2, 768], P('section'), may hold values from 0 to 3, never falling along the last dimension, each value on 1 to 384 neighbouring positions
Outputs:
- forward_out: bfloat16 [16, 768, 4096], P('section', 'tp')
- backward_out: bfloat16 [16, 768, 4096], P('section', 'tp')
The draws below stay inside these ranges and needn't reach their ends.
Inputs may be any that keep to these rules, and one draw needn't show every extreme that they name: `modality`: 0 marks a text token and 1 an image token; image tokens come in runs of positions, and both modalities occur in every micro-batch. `documents`: document numbers start at 0 and never fall along the positions of a micro-batch.
All inputs are finite; a program needn't handle non-finite values.
Results may differ from the reference program's by a relative error of at most 0.014.
Values may be sent and summed in bfloat16 or wider, within the bound.
A program may use at most 128 MiB of HBM per device.

```python
import math
import jax
import jax.numpy as jnp
import numpy as np
from jax import lax

D = 4096
HEADS = 16
HEAD_DIM = 128
SECTIONS = 16
TOKENS = 768
N_TP = 16


def activation_draw(key, shape):
    rows_key, columns_key, noise_key = jax.random.split(key, 3)
    leading = shape[:-1] + (1,)
    width = shape[-1]
    row_scale = jnp.exp(jax.random.uniform(rows_key, leading, jnp.float32, math.log(0.2), math.log(2.0)))
    column_scale = jnp.exp(jax.random.uniform(columns_key, (width,), jnp.float32, math.log(0.25), math.log(2.5)))
    base = jnp.clip(jax.random.normal(noise_key, shape, jnp.float32), -4.0, 4.0)
    return (base * row_scale * column_scale).astype(jnp.bfloat16)


def draw_embedded(key, part):
    return activation_draw(jax.random.fold_in(key, 11), (TOKENS, D))


def draw_previous_out(key, part):
    return activation_draw(jax.random.fold_in(key, 12), (SECTIONS, TOKENS, D))


def draw_saved_input(key, part):
    return activation_draw(jax.random.fold_in(key, 13), (SECTIONS, TOKENS, D))


def draw_saved_qkv(key, part):
    first_key, second_key, third_key = jax.random.split(jax.random.fold_in(key, 14), 3)
    shape = (SECTIONS, TOKENS, HEADS * HEAD_DIM)
    queries = jnp.clip(jax.random.normal(first_key, shape, jnp.float32), -4.0, 4.0)
    keys = jnp.clip(jax.random.normal(second_key, shape, jnp.float32), -4.0, 4.0)
    values = jnp.clip(jax.random.normal(third_key, shape, jnp.float32), -4.0, 4.0)
    return jnp.stack([queries, keys, values], axis=2).astype(jnp.bfloat16)


def draw_qkv_weight(key, part):
    first_key, second_key, third_key = jax.random.split(jax.random.fold_in(key, 15), 3)
    shape = (SECTIONS, 2, D, HEADS * HEAD_DIM)
    spread = D ** (-0.5)
    queries = jnp.clip(jax.random.normal(first_key, shape, jnp.float32), -4.0, 4.0) * spread
    noise = jnp.clip(jax.random.normal(second_key, shape, jnp.float32), -4.0, 4.0) * spread
    values = jnp.clip(jax.random.normal(third_key, shape, jnp.float32), -4.0, 4.0) * spread
    keys = noise
    return jnp.stack([queries, keys, values], axis=3).astype(jnp.bfloat16)


def draw_modality(key, part):
    start_key, length_key = jax.random.split(jax.random.fold_in(key, 16), 2)
    starts = jax.random.randint(start_key, (SECTIONS, 2, 3), 0, TOKENS)
    spans = jax.random.randint(length_key, (SECTIONS, 2, 3), max(TOKENS // 16, 1), TOKENS // 4 + 1)
    position = jnp.arange(TOKENS, dtype=jnp.int32)
    inside = (position >= starts[..., None]) & (position < starts[..., None] + spans[..., None])
    return jnp.any(inside, axis=2).astype(jnp.int32)


def block_scale(stream_key, extent, cuts, smallest, high):
    gain = 1.0
    for dim, shards_of in cuts:
        heights = jax.random.uniform(jax.random.fold_in(jax.random.fold_in(stream_key, 6), dim), (shards_of,), jnp.float32, smallest / len(cuts), high / len(cuts))
        gain = gain * jnp.repeat(jnp.exp(heights), extent[dim] // shards_of).reshape((-1,) + (1,) * (len(extent) - 1 - dim))
    return gain


def profile(number_of, total, bound, skew):
    portions = [(1 << 20) // math.isqrt(grade ** skew) + 1 for grade in range(2, number_of + 1)]
    rest, holding = total - bound - (number_of - 1), [1] * (number_of - 1)
    while rest > 0:
        movable = [i for i in range(number_of - 1) if holding[i] < bound]
        whole, budget = sum([portions[i] for i in movable]), rest
        for i in movable:
            extra = min(bound - holding[i], max(1, budget * portions[i] // whole), rest)
            holding[i] = holding[i] + extra
            rest = rest - extra
    return np.array([bound] + holding)


def uneven_parts(rng, count, total, reach, skew):
    if count == 2:
        one = jax.random.randint(rng, (), max(1, total - reach), min(reach, total - 1) + 1)
        return jnp.stack([one, total - one])
    tallies = jnp.asarray(profile(count, total, reach, skew), jnp.int32)
    couples = (count - 1) // 2
    donor, receiver = tallies[1:1 + 2 * couples:2], tallies[2:2 + 2 * couples:2]
    margin = jnp.minimum(donor - 1, reach - receiver)
    shifted = jax.random.randint(jax.random.fold_in(rng, 1), (couples,), 0, 1 << 20) % (margin + 1)
    tallies = tallies.at[1:1 + 2 * couples:2].set(donor - shifted).at[2:2 + 2 * couples:2].set(receiver + shifted)
    return tallies[jax.random.permutation(jax.random.fold_in(rng, 2), count)]


def gaussian(stream_key, extent, scale, limit, shards=(), held_as=jnp.bfloat16):
    entries = jax.random.normal(stream_key, extent, jnp.float32) * scale
    if len(shards) > 0:
        entries = block_scale(stream_key, extent, shards, -0.22, 0.18) * entries
    return jnp.clip(entries, min=-limit, max=limit).astype(held_as)


def setup_inputs(seed: int = 0) -> dict:
    seeds = jax.random.split(jax.random.key(seed), 12)
    return {
        "embedded": draw_embedded(jax.random.fold_in(seeds[11], 71), 0),
        "previous_out": draw_previous_out(jax.random.fold_in(seeds[11], 71), 0),
        "top_grad": gaussian(seeds[2], (TOKENS, D), 1.0, 6.0, ((0, 16),)),
        "grad_out": gaussian(seeds[3], (SECTIONS, TOKENS, D), 1.0, 6.0, ((0, 16), (1, 16))),
        "saved_input": draw_saved_input(jax.random.fold_in(seeds[11], 71), 0),
        "saved_qkv": draw_saved_qkv(jax.random.fold_in(seeds[11], 71), 0),
        "norm_gain": jnp.clip(1.0 + 0.18 * jax.random.normal(seeds[6], (SECTIONS, 2, D), jnp.float32), 0.1, 1.9),
        "qkv_weight": draw_qkv_weight(jax.random.fold_in(seeds[11], 71), 0),
        "out_weight": gaussian(seeds[8], (SECTIONS, 2, HEADS * HEAD_DIM, D), (HEADS * HEAD_DIM) ** -0.5, 0.125, ((0, 16), (2, 16))),
        "modality": draw_modality(jax.random.fold_in(seeds[11], 71), 0),
        "documents": jax.vmap(lambda own: jnp.searchsorted(jnp.cumsum(uneven_parts(own, 4, TOKENS, TOKENS // 2, 0)), jnp.arange(TOKENS), side="right"))(jax.random.split(seeds[10], SECTIONS * 2)).reshape((SECTIONS, 2, TOKENS)).astype(jnp.int32),
    }


EPSILON = 1e-05

def by_modality(rows, labels, weights, side):
    numbers = (((1,), (side,)), ((), ()))
    first = lax.dot_general(rows, weights[0], numbers, preferred_element_type=jnp.float32)
    second = lax.dot_general(rows, weights[1], numbers, preferred_element_type=jnp.float32)
    return jnp.where(labels[:, None] == 0, first, second)

def gain_rows(gains, labels):
    return jnp.where(labels[:, None] == 0, gains[0][None, :], gains[1][None, :])

def probabilities(queries, keys, documents_row):
    length = queries.shape[0]
    scores = jnp.einsum('thd,shd->hts', queries.astype(jnp.float32), keys.astype(jnp.float32)) / math.sqrt(HEAD_DIM)
    position = jnp.arange(length, dtype=jnp.int32)
    allowed = (position[None, :] <= position[:, None]) & (documents_row[:, None] == documents_row[None, :])
    scores = jnp.where(allowed[None, :, :], scores, -jnp.inf)
    highest = lax.optimization_barrier(jnp.max(scores, axis=-1, keepdims=True))
    weights = jnp.exp(scores - highest)
    return weights / lax.optimization_barrier(jnp.sum(weights, axis=-1, keepdims=True))

def one_section(items):
    inputs, upstream, saved_rows, saved, gains, w_project, w_output, labels, documents_pair = items
    length = inputs.shape[0]
    group = HEADS * HEAD_DIM // N_TP
    labels_fwd = labels[0]
    labels_back = labels[1]
    forward_rows = inputs.astype(jnp.float32)
    inverse = lax.rsqrt(lax.optimization_barrier(jnp.mean(forward_rows * forward_rows, axis=-1, keepdims=True)) + EPSILON)
    normed = (forward_rows * inverse * gain_rows(gains, labels_fwd)).astype(jnp.bfloat16)
    flat_weight = w_project.reshape(2, D, 3 * HEADS * HEAD_DIM)
    projected = lax.optimization_barrier(by_modality(normed, labels_fwd, flat_weight, 0).astype(jnp.bfloat16))
    projected = projected.reshape(length, 3, HEADS, HEAD_DIM)
    probs = lax.optimization_barrier(probabilities(projected[:, 0], projected[:, 1], documents_pair[0]).astype(jnp.bfloat16))
    attended = jnp.einsum('hts,shd->thd', probs.astype(jnp.float32), projected[:, 2].astype(jnp.float32))
    attended = attended.astype(jnp.bfloat16).reshape(length, HEADS * HEAD_DIM)

    def add_output(index, total):
        begin = (index * group).astype(jnp.int32)
        rows = lax.dynamic_slice_in_dim(attended, begin, group, 1)
        weights = lax.dynamic_slice_in_dim(w_output, begin, group, 1)
        term = by_modality(rows, labels_fwd, weights, 0)
        return total + lax.optimization_barrier(term.astype(jnp.bfloat16)).astype(jnp.float32)
    mixed = lax.fori_loop(0, N_TP, add_output, jnp.zeros((length, D), jnp.float32))
    forward_out = (forward_rows + mixed).astype(jnp.bfloat16)
    grad_attended = lax.optimization_barrier(by_modality(upstream, labels_back, w_output, 1).astype(jnp.bfloat16))
    grad_attended = grad_attended.astype(jnp.float32).reshape(length, HEADS, HEAD_DIM)
    stored = saved.reshape(length, 3, HEADS, HEAD_DIM)
    queries = stored[:, 0].astype(jnp.float32)
    keys = stored[:, 1].astype(jnp.float32)
    values = stored[:, 2].astype(jnp.float32)
    probs_back = probabilities(stored[:, 0], stored[:, 1], documents_pair[1])
    rounded = lax.optimization_barrier(probs_back.astype(jnp.bfloat16)).astype(jnp.float32)
    grad_values = jnp.einsum('hts,thd->shd', rounded, grad_attended).astype(jnp.bfloat16)
    grad_probs = jnp.einsum('thd,shd->hts', grad_attended, values)
    delta = lax.optimization_barrier(jnp.sum(probs_back * grad_probs, axis=-1, keepdims=True))
    grad_scores = lax.optimization_barrier((probs_back * (grad_probs - delta) / math.sqrt(HEAD_DIM)).astype(jnp.bfloat16))
    grad_scores = grad_scores.astype(jnp.float32)
    grad_queries = jnp.einsum('hts,shd->thd', grad_scores, keys).astype(jnp.bfloat16)
    grad_keys = jnp.einsum('hts,thd->shd', grad_scores, queries).astype(jnp.bfloat16)
    grads = jnp.stack([grad_queries, grad_keys, grad_values], axis=1).reshape(length, 3, HEADS * HEAD_DIM)

    def add_input(index, total):
        begin = (index * group).astype(jnp.int32)
        rows = lax.dynamic_slice_in_dim(grads, begin, group, 2).reshape(length, 3 * group)
        weights = lax.dynamic_slice_in_dim(w_project, begin, group, 3).reshape(2, D, 3 * group)
        term = by_modality(rows, labels_back, weights, 1)
        return total + lax.optimization_barrier(term.astype(jnp.bfloat16)).astype(jnp.float32)
    grad_normed = lax.fori_loop(0, N_TP, add_input, jnp.zeros((length, D), jnp.float32))
    back_rows = saved_rows.astype(jnp.float32)
    inverse_back = lax.rsqrt(lax.optimization_barrier(jnp.mean(back_rows * back_rows, axis=-1, keepdims=True)) + EPSILON)
    scaled = grad_normed * gain_rows(gains, labels_back)
    correction = lax.optimization_barrier(jnp.mean(scaled * back_rows, axis=-1, keepdims=True))
    norm_grad = inverse_back * scaled - back_rows * inverse_back * inverse_back * inverse_back * correction
    backward_out = (upstream.astype(jnp.float32) + norm_grad).astype(jnp.bfloat16)
    return (forward_out, backward_out)

def reference(embedded, previous_out, top_grad, grad_out, saved_input, saved_qkv, norm_gain, qkv_weight, out_weight, modality, documents):
    inputs = jnp.concatenate([embedded[None], previous_out[:-1]], axis=0)
    upstream = jnp.concatenate([grad_out[1:], top_grad[None]], axis=0)
    forward_out, backward_out = lax.map(one_section, (inputs, upstream, saved_input, saved_qkv, norm_gain, qkv_weight, out_weight, modality, documents))
    return (forward_out, backward_out)
```

```python
import functools
import math

import jax
import jax.numpy as jnp
from jax import lax
from jax.experimental import pallas as pl
from jax.experimental.pallas import tpu as pltpu
from jax.sharding import PartitionSpec as P

EPSILON = 1e-05
HEAD_DIM = 128
MESH = pl.DeviceIdType.MESH
BF = jnp.bfloat16
F32 = jnp.float32
QB = 256


def nt(x, y):
    return lax.dot_general(x, y, (((1,), (1,)), ((), ())), preferred_element_type=F32)


def tn(x, y):
    return lax.dot_general(x, y, (((0,), (0,)), ((), ())), preferred_element_type=F32)


def nn(x, y):
    return jnp.dot(x, y, preferred_element_type=F32)


class Sems:
    def __init__(self, send, recv):
        self.send, self.recv, self.count, self.open = send, recv, 0, []

    def copy(self, src, dst, peer):
        i = self.count
        self.count += 1
        c = pltpu.make_async_remote_copy(
            src_ref=src, dst_ref=dst, send_sem=self.send.at[i], recv_sem=self.recv.at[i],
            device_id=peer, device_id_type=MESH,
        )
        c.start()
        self.open.append(c)
        return i

    def landed(self, ref, i, peer):
        pltpu.make_async_remote_copy(
            src_ref=ref, dst_ref=ref, send_sem=self.send.at[i], recv_sem=self.recv.at[i],
            device_id=peer, device_id_type=MESH,
        ).wait_recv()

    def drain(self):
        for c in self.open:
            c.wait_send()


N_SEMS = 112
N_LOCAL = 16


def kernel(
    emb, prev, topg, gout, sin, sqkv, gain, wq, wo, mod, doc,
    fout, bout,
    w1, wor, inp, embv, ups, topv, sinv, qkvv, ag, proj, attg, op, oz1, oz2, fo, fa,
    u, gap, gar, gat, pb, ds, dkv, gr, g, gx1, gx2, sx, gz1, gz2, lt, dt, acc,
    ssem, rsem, lsem,
):
    s = lax.axis_index("section")
    t = lax.axis_index("tp")
    n_sec = lax.axis_size("section")
    a, b = t % 4, t // 4
    aR, aL, aO = (a + 1) % 4, (a + 3) % 4, (a + 2) % 4
    bR, bL, bO = (b + 1) % 4, (b + 3) % 4, (b + 2) % 4
    XR, XL, XO = (s, 4 * b + aR), (s, 4 * b + aL), (s, 4 * b + aO)
    ZR, ZL = (s, 4 * bR + a), (s, 4 * bL + a)
    SR, SL = ((s + 1) % n_sec, t), ((s + n_sec - 1) % n_sec, t)
    rows = inp.shape[0]
    width = inp.shape[1]
    half = width // 2
    quarter = width // 4
    length = ag.shape[0] * rows
    chunk = 4 * rows
    scale = 1.0 / math.sqrt(HEAD_DIM)

    bar = pltpu.get_barrier_semaphore()
    for peer in (SR, SL, XR, XL, XO, ZR, ZL):
        pl.semaphore_signal(bar, inc=1, device_id=peer, device_id_type=MESH)
    pl.semaphore_wait(bar, 7)

    q = Sems(ssem, rsem)
    local = []

    def fetch(src, dst):
        c = pltpu.make_async_copy(src, dst, lsem.at[len(local)])
        c.start()
        local.append(c)
        return c

    i_shift_f = q.copy(prev, inp, SR)
    i_shift_b = q.copy(gout, ups, SL)

    def regroup(m):
        mine = fetch(wo.at[m, :, pl.ds(pl.multiple_of(a * quarter, quarter), quarter)], wor.at[m, a])
        ids = []
        for peer, col in ((XR, aR), (XL, aL), (XO, aO)):
            src = wo.at[m, :, pl.ds(pl.multiple_of(col * quarter, quarter), quarter)]
            ids.append(q.copy(src, wor.at[m, a], peer))
        return mine, ids

    f_qkv = fetch(sqkv, qkvv)
    f_emb = fetch(emb, embv)
    f_top = fetch(topg, topv)
    f_sin = fetch(sin, sinv)
    wo0 = regroup(0)
    f_w1 = [
        fetch(wq.at[m, j], w1.at[:, pl.ds(m * 384 + j * 128, 128)]) for m in range(2) for j in range(3)
    ]

    for k in range(2):
        lt[k] = jnp.broadcast_to(mod[k : k + 1, :].astype(F32), (128, length)).T
        dt[k] = jnp.broadcast_to(doc[k : k + 1, :].astype(F32), (128, length)).T

    def softmax_block(qb, kb, which, i):
        n = (i + 1) * QB
        sc = nt(qb, kb) * scale
        qpos = lax.broadcasted_iota(jnp.int32, (QB, n), 0) + i * QB
        kpos = lax.broadcasted_iota(jnp.int32, (QB, n), 1)
        dq = dt[which, i * QB : (i + 1) * QB, 0:1]
        dk = doc[which : which + 1, 0:n].astype(F32)
        sc = jnp.where((kpos <= qpos) & (dq == dk), sc, -jnp.inf)
        e = jnp.exp(sc - jnp.max(sc, axis=-1, keepdims=True))
        return e / jnp.sum(e, axis=-1, keepdims=True)

    n_blocks = length // QB

    def saved_probs():
        for i in range(n_blocks):
            pb[i * QB : (i + 1) * QB, 0 : (i + 1) * QB] = softmax_block(
                qkvv[0, i * QB : (i + 1) * QB, :], qkvv[1, 0 : (i + 1) * QB, :], 1, i
            )

    f_qkv.wait()
    f_emb.wait()
    f_top.wait()

    q.landed(inp, i_shift_f, SL)

    def norm_rows(r, _):
        r0 = pl.multiple_of(r * 16, 16)
        x = jnp.where(s == 0, embv[pl.ds(r0, 16), :], inp[pl.ds(r0, 16), :])
        inp[pl.ds(r0, 16), :] = x
        x = x.astype(F32)
        inv = lax.rsqrt(jnp.mean(x * x, axis=-1, keepdims=True) + EPSILON)
        lab = lt[0, pl.ds(pl.multiple_of(t * rows + r0, 16), 16), 0:1]
        gn = jnp.where(lab == 0.0, gain[0:1, :], gain[1:2, :])
        ag[t, pl.ds(r0, 16), :] = (x * inv * gn).astype(BF)
        return 0

    lax.fori_loop(0, rows // 16, norm_rows, 0)
    i_nz = q.copy(ag.at[t], ag.at[t], ZR), q.copy(ag.at[t], ag.at[t], ZL)

    q.landed(ups, i_shift_b, SR)

    def up_rows(r, _):
        r0 = pl.multiple_of(r * 16, 16)
        x = jnp.where(s == n_sec - 1, topv[pl.ds(r0, 16), :], ups[pl.ds(r0, 16), :])
        ups[pl.ds(r0, 16), :] = x
        return 0

    lax.fori_loop(0, rows // 16, up_rows, 0)
    mine_rows = pl.ds(pl.multiple_of(a * rows, rows), rows)
    i_up = []
    for peer, col in ((XR, aR), (XL, aL), (XO, aO)):
        src = ups.at[:, pl.ds(pl.multiple_of(col * quarter, quarter), quarter)]
        i_up.append(q.copy(src, u.at[b, mine_rows, :], peer))
    u[b, mine_rows, :] = ups[:, pl.ds(pl.multiple_of(a * quarter, quarter), quarter)]
    wo1 = regroup(1)
    i_nx = {}

    def spread_x(key, slot):
        i_nx[key] = q.copy(ag.at[slot], ag.at[slot], XR), q.copy(ag.at[slot], ag.at[slot], XL)

    spread_x("B", t)
    saved_probs()

    for (i, peer, src_a) in zip(i_up, (XL, XR, XO), (aL, aR, aO)):
        q.landed(u.at[b, pl.ds(pl.multiple_of(src_a * rows, rows), rows), :], i, peer)
    i_uz = q.copy(u.at[b], u.at[b], ZR), q.copy(u.at[b], u.at[b], ZL)

    h0, h1 = pl.ds(0, half), pl.ds(half, half)
    slotL, slotR, slotO = 4 * bL + a, 4 * bR + a, 4 * bO + a
    q.landed(ag.at[slotL], i_nz[0], ZL)
    i_nzf0 = q.copy(ag.at[slotL, :, h0], ag.at[slotL, :, h0], ZR)
    spread_x("L", slotL)
    q.landed(ag.at[slotR], i_nz[1], ZR)
    i_nzf1 = q.copy(ag.at[slotR, :, h1], ag.at[slotR, :, h1], ZL)
    spread_x("R", slotR)

    i_nxf = {}

    def forward_x(key, bb):
        sl, sr = 4 * bb + aL, 4 * bb + aR
        q.landed(ag.at[sl], i_nx[key][0], XL)
        i0 = q.copy(ag.at[sl, :, h0], ag.at[sl, :, h0], XR)
        q.landed(ag.at[sr], i_nx[key][1], XR)
        i1 = q.copy(ag.at[sr, :, h1], ag.at[sr, :, h1], XL)
        i_nxf[key] = i0, i1

    def complete_x(key, bb):
        so = 4 * bb + aO
        q.landed(ag.at[so, :, h0], i_nxf[key][0], XL)
        q.landed(ag.at[so, :, h1], i_nxf[key][1], XR)

    KT = 512

    def project(bb):
        acc[...] = jnp.zeros_like(acc)

        def step(k, _):
            k0 = pl.ds(pl.multiple_of(k * KT, KT), KT)
            x = ag[pl.ds(4 * bb, 4), :, k0].reshape(chunk, KT)
            acc[...] += nn(x, w1[k0, :])
            return 0

        lax.fori_loop(0, width // KT, step, 0)
        r = pl.ds(pl.multiple_of(bb * chunk, chunk), chunk)
        lab = lt[0, r, 0:1]
        proj[r, :] = jnp.where(lab == 0.0, acc[:, 0:384], acc[:, 384:768]).astype(BF)

    forward_x("B", b)

    qh0, qh1 = pl.ds(0, quarter // 2), pl.ds(quarter // 2, quarter // 2)
    q.landed(u.at[bL], i_uz[0], ZL)
    i_uzf0 = q.copy(u.at[bL, :, qh0], u.at[bL, :, qh0], ZR)
    q.landed(u.at[bR], i_uz[1], ZR)
    i_uzf1 = q.copy(u.at[bR, :, qh1], u.at[bR, :, qh1], ZL)

    for c in f_w1:
        c.wait()
    complete_x("B", b)
    project(b)

    for mine, ids in (wo0, wo1):
        mine.wait()
    for m, (mine, ids) in enumerate((wo0, wo1)):
        for i, peer, src_a in zip(ids, (XL, XR, XO), (aL, aR, aO)):
            q.landed(wor.at[m, src_a], i, peer)

    def grad_att(bb):
        r = pl.ds(pl.multiple_of(bb * chunk, chunk), chunk)
        lab = lt[1, r, 0:1]
        x = u[bb]
        for hp in range(2):
            y0 = nt(x, wor[0, 2 * hp : 2 * hp + 2].reshape(256, quarter))
            y1 = nt(x, wor[1, 2 * hp : 2 * hp + 2].reshape(256, quarter))
            y = jnp.where(lab == 0.0, y0, y1).astype(BF)
            gap[2 * hp, r, :] = y[:, 0:128]
            gap[2 * hp + 1, r, :] = y[:, 128:256]

    grad_att(b)
    grad_att(bL)
    grad_att(bR)

    q.landed(ag.at[slotO, :, h0], i_nzf0, ZL)
    q.landed(ag.at[slotO, :, h1], i_nzf1, ZR)
    forward_x("L", bL)
    spread_x("O", slotO)

    q.landed(u.at[bO, :, qh0], i_uzf0, ZL)
    q.landed(u.at[bO, :, qh1], i_uzf1, ZR)
    grad_att(bO)
    i_ga = [q.copy(gap.at[k], gar.at[a], peer) for peer, k in ((XR, aR), (XL, aL), (XO, aO))]
    forward_x("R", bR)
    complete_x("L", bL)
    project(bL)

    for i, peer, src_a in zip(i_ga, (XL, XR, XO), (aL, aR, aO)):
        q.landed(gar.at[src_a], i, peer)

    def sum_ga(r, _):
        rr = pl.ds(pl.multiple_of(r * 64, 64), 64)
        total = gap[a, rr, :].astype(F32) + gar[aL, rr, :].astype(F32)
        total += gar[aR, rr, :].astype(F32) + gar[aO, rr, :].astype(F32)
        gat[rr, :] = total.astype(BF)
        return 0

    lax.fori_loop(0, length // 64, sum_ga, 0)

    for i in range(n_blocks):
        r = slice(i * QB, (i + 1) * QB)
        n = (i + 1) * QB
        p = pb[r, 0:n]
        gp = nt(gat[r, :], qkvv[2, 0:n, :])
        delta = jnp.sum(p * gp, axis=-1, keepdims=True)
        d = (p * (gp - delta) * scale).astype(BF)
        ds[r, 0:n] = d
        dq = nn(d, qkvv[1, 0:n, :]).astype(BF)
        lab = lt[1, r, 0:1]
        zero = jnp.zeros_like(dq)
        gr[r, 0:128] = jnp.where(lab == 0.0, dq, zero)
        gr[r, 384:512] = jnp.where(lab == 0.0, zero, dq)
    for j in range(n_blocks):
        cols = slice(j * QB, (j + 1) * QB)
        dk = jnp.zeros((QB, HEAD_DIM), F32)
        dv = jnp.zeros((QB, HEAD_DIM), F32)
        for i in range(j, n_blocks):
            r = slice(i * QB, (i + 1) * QB)
            dk += tn(ds[r, cols], qkvv[0, r, :])
            dv += tn(pb[r, cols].astype(BF), gat[r, :])
        lab = lt[1, cols, 0:1]
        zero = jnp.zeros((QB, HEAD_DIM), BF)
        gr[cols, 128:256] = jnp.where(lab == 0.0, dk.astype(BF), zero)
        gr[cols, 512:640] = jnp.where(lab == 0.0, zero, dk.astype(BF))
        gr[cols, 256:384] = jnp.where(lab == 0.0, dv.astype(BF), zero)
        gr[cols, 640:768] = jnp.where(lab == 0.0, zero, dv.astype(BF))

    def grad_in(bb):
        r = pl.ds(pl.multiple_of(bb * chunk, chunk), chunk)

        def step(k, _):
            k0 = pl.ds(pl.multiple_of(k * KT, KT), KT)
            y = nt(gr[r, :], w1[k0, :]).astype(BF)
            g[pl.ds(4 * bb, 4), :, k0] = y.reshape(4, rows, KT)
            return 0

        lax.fori_loop(0, width // KT, step, 0)

    order = [bO, bR, bL, b]
    i_gx = {}

    def gx_send(k):
        bb = order[k]
        o, l, r = 4 * bb + aO, 4 * bb + aL, 4 * bb + aR
        i_gx[k] = [
            q.copy(g.at[o, :, h0], gx1.at[k, 0], XL),
            q.copy(g.at[o, :, h1], gx1.at[k, 1], XR),
            q.copy(g.at[l, :, h1], gx2.at[k, 0, :, h1], XL),
            q.copy(g.at[r, :, h0], gx2.at[k, 1, :, h0], XR),
        ]

    def gx_pass(k):
        bb = order[k]
        l, r = 4 * bb + aL, 4 * bb + aR
        q.landed(gx1.at[k, 0], i_gx[k][0], XR)
        g[l, :, h0] = (g[l, :, h0].astype(F32) + gx1[k, 0].astype(F32)).astype(BF)
        i0 = q.copy(g.at[l, :, h0], gx2.at[k, 0, :, h0], XL)
        q.landed(gx1.at[k, 1], i_gx[k][1], XL)
        g[r, :, h1] = (g[r, :, h1].astype(F32) + gx1[k, 1].astype(F32)).astype(BF)
        i1 = q.copy(g.at[r, :, h1], gx2.at[k, 1, :, h1], XR)
        i_gx[k] += [i0, i1]

    def gx_sum(k):
        ids = i_gx[k]
        q.landed(gx2.at[k, 0, :, h1], ids[2], XR)
        q.landed(gx2.at[k, 1, :, h0], ids[3], XL)
        q.landed(gx2.at[k, 0, :, h0], ids[4], XR)
        q.landed(gx2.at[k, 1, :, h1], ids[5], XL)
        own = 4 * order[k] + a

        def step(c, _):
            c0 = pl.ds(pl.multiple_of(c * KT, KT), KT)
            total = g[own, :, c0].astype(F32) + gx2[k, 0, :, c0].astype(F32) + gx2[k, 1, :, c0].astype(F32)
            sx[k, :, c0] = total.astype(BF)
            return 0

        lax.fori_loop(0, width // KT, step, 0)

    grad_in(order[0])
    gx_send(0)

    forward_x("O", bO)
    complete_x("R", bR)
    project(bR)
    gx_pass(0)
    grad_in(order[1])
    gx_send(1)
    complete_x("O", bO)
    project(bO)

    for i in range(n_blocks):
        r = slice(i * QB, (i + 1) * QB)
        n = (i + 1) * QB
        p = softmax_block(proj[r, 0:128], proj[0:n, 128:256], 0, i).astype(BF)
        attg[a, r, :] = nn(p, proj[0:n, 256:384]).astype(BF)
    i_at = [q.copy(attg.at[a], attg.at[a], peer) for peer in (XR, XL, XO)]

    gx_pass(1)
    grad_in(order[2])
    gx_send(2)
    gx_sum(0)
    i_gz1 = [q.copy(sx.at[0, :, h0], gz1.at[0], ZL), q.copy(sx.at[0, :, h1], gz1.at[1], ZR)]

    for i, peer, src_a in zip(i_at, (XL, XR, XO), (aL, aR, aO)):
        q.landed(attg.at[src_a], i, peer)

    def out_proj(bb, k):
        r = pl.ds(pl.multiple_of(bb * chunk, chunk), chunk)
        lab = lt[0, r, 0:1]
        heads = [attg[h, r, :] for h in range(4)]
        zero = jnp.zeros((chunk, HEAD_DIM), BF)
        x = jnp.concatenate(
            [jnp.where(lab == 0.0, h, zero) for h in heads] + [jnp.where(lab == 0.0, zero, h) for h in heads], axis=1
        )
        for c in range(2):
            y = wor[:, :, :, c * 512 : (c + 1) * 512].reshape(1024, 512)
            op[k, :, c * 512 : (c + 1) * 512] = nn(x, y).astype(BF)

    out_proj(bO, 0)
    i_oz = [q.copy(op.at[0, :, qh0], oz1.at[0], ZL), q.copy(op.at[0, :, qh1], oz1.at[1], ZR)]
    out_proj(bR, 1)
    i_oz.append(q.copy(op.at[1, :, qh0], oz2.at[1, :, qh0], ZR))
    out_proj(bL, 2)
    i_oz.append(q.copy(op.at[2, :, qh1], oz2.at[0, :, qh1], ZL))
    out_proj(b, 3)

    gx_pass(2)
    grad_in(order[3])
    gx_send(3)

    gx_sum(1)
    i_gz2 = [q.copy(sx.at[1, :, h0], gz2.at[1, :, h0], ZR)]

    q.landed(oz1.at[0], i_oz[0], ZR)
    op[2, :, qh0] = (op[2, :, qh0].astype(F32) + oz1[0].astype(F32)).astype(BF)
    i_oz.append(q.copy(op.at[2, :, qh0], oz2.at[0, :, qh0], ZL))
    q.landed(oz1.at[1], i_oz[1], ZL)
    op[1, :, qh1] = (op[1, :, qh1].astype(F32) + oz1[1].astype(F32)).astype(BF)
    i_oz.append(q.copy(op.at[1, :, qh1], oz2.at[1, :, qh1], ZR))

    gx_pass(3)
    gx_sum(2)
    i_gz2.append(q.copy(sx.at[2, :, h1], gz2.at[0, :, h1], ZL))

    q.landed(gz1.at[0], i_gz1[0], ZR)
    sx[2, :, h0] = (sx[2, :, h0].astype(F32) + gz1[0].astype(F32)).astype(BF)
    i_gz2.append(q.copy(sx.at[2, :, h0], gz2.at[0, :, h0], ZL))
    q.landed(gz1.at[1], i_gz1[1], ZL)
    sx[1, :, h1] = (sx[1, :, h1].astype(F32) + gz1[1].astype(F32)).astype(BF)
    i_gz2.append(q.copy(sx.at[1, :, h1], gz2.at[1, :, h1], ZR))

    q.landed(oz2.at[1, :, qh0], i_oz[2], ZL)
    q.landed(oz2.at[0, :, qh1], i_oz[3], ZR)
    q.landed(oz2.at[0, :, qh0], i_oz[4], ZR)
    q.landed(oz2.at[1, :, qh1], i_oz[5], ZL)

    def sum_out(k, _):
        rr = pl.ds(pl.multiple_of(k * rows, rows), rows)
        total = op[3, rr, :].astype(F32) + oz2[0, rr, :].astype(F32) + oz2[1, rr, :].astype(F32)
        fo[k] = total.astype(BF)
        return 0

    lax.fori_loop(0, 4, sum_out, 0)
    i_fa = [q.copy(fo.at[k], fa.at[a], peer) for peer, k in ((XR, aR), (XL, aL), (XO, aO))]
    fa[a] = fo[a]

    f_sin.wait()
    gx_sum(3)

    for i, peer, src_a in zip(i_fa, (XL, XR, XO), (aL, aR, aO)):
        q.landed(fa.at[src_a], i, peer)
    for k in range(4):
        cols = slice(k * quarter, (k + 1) * quarter)
        fout[:, cols] = (inp[:, cols].astype(F32) + fa[k].astype(F32)).astype(BF)

    q.landed(gz2.at[1, :, h0], i_gz2[0], ZL)
    q.landed(gz2.at[0, :, h1], i_gz2[1], ZR)
    q.landed(gz2.at[0, :, h0], i_gz2[2], ZR)
    q.landed(gz2.at[1, :, h1], i_gz2[3], ZL)

    def back_rows(r, _):
        rr = pl.ds(pl.multiple_of(r * 16, 16), 16)
        total = sx[3, rr, :].astype(F32) + gz2[0, rr, :].astype(F32) + gz2[1, rr, :].astype(F32)
        lab = lt[1, pl.ds(pl.multiple_of(t * rows + r * 16, 16), 16), 0:1]
        scaled = total * jnp.where(lab == 0.0, gain[0:1, :], gain[1:2, :])
        x = sinv[rr, :].astype(F32)
        inv = lax.rsqrt(jnp.mean(x * x, axis=-1, keepdims=True) + EPSILON)
        corr = jnp.mean(scaled * x, axis=-1, keepdims=True)
        bout[rr, :] = (ups[rr, :].astype(F32) + inv * scaled - x * inv * inv * inv * corr).astype(BF)
        return 0

    lax.fori_loop(0, rows // 16, back_rows, 0)
    q.drain()


def body(
    embedded, previous_out, top_grad, grad_out, saved_input, saved_qkv, norm_gain, qkv_weight, out_weight,
    modality, documents,
):
    rows, width = embedded.shape
    length = saved_qkv.shape[1]
    blocks = length // rows
    quarter = width // 4
    wq = jnp.transpose(qkv_weight[0], (0, 2, 1, 3))
    sqkv = jnp.transpose(saved_qkv[0], (1, 0, 2))
    vm = pl.BlockSpec(memory_space=pltpu.VMEM)
    hb = pl.BlockSpec(memory_space=pl.ANY)
    v = pltpu.VMEM
    out = jax.ShapeDtypeStruct((rows, width), BF)
    chunk = 4 * rows
    fwd, bwd = pl.pallas_call(
        kernel,
        out_shape=(out, out),
        in_specs=[hb, hb, hb, hb, hb, hb, vm, hb, hb, vm, vm],
        out_specs=(vm, vm),
        scratch_shapes=[
            v((width, 768), BF),
            v((2, 4, 128, quarter), BF),
            v((rows, width), BF),
            v((rows, width), BF),
            v((rows, width), BF),
            v((rows, width), BF),
            v((rows, width), BF),
            v((3, length, HEAD_DIM), BF),
            v((blocks, rows, width), BF),
            v((length, 384), BF),
            v((4, length, HEAD_DIM), BF),
            v((4, chunk, quarter), BF),
            v((2, chunk, quarter // 2), BF),
            v((2, chunk, quarter), BF),
            v((4, rows, quarter), BF),
            v((4, rows, quarter), BF),
            v((4, chunk, quarter), BF),
            v((4, length, HEAD_DIM), BF),
            v((4, length, HEAD_DIM), BF),
            v((length, HEAD_DIM), BF),
            v((length, length), F32),
            v((length, length), BF),
            v((8, 128), F32),
            v((length, 768), BF),
            v((blocks, rows, width), BF),
            v((4, 2, rows, width // 2), BF),
            v((4, 2, rows, width), BF),
            v((4, rows, width), BF),
            v((2, rows, width // 2), BF),
            v((2, rows, width), BF),
            v((2, length, 128), F32),
            v((2, length, 128), F32),
            v((chunk, 768), F32),
            pltpu.SemaphoreType.DMA((N_SEMS,)),
            pltpu.SemaphoreType.DMA((N_SEMS,)),
            pltpu.SemaphoreType.DMA((N_LOCAL,)),
        ],
        compiler_params=pltpu.CompilerParams(
            collective_id=0, has_side_effects=True, vmem_limit_bytes=62 * 1024 * 1024
        ),
        name="relay",
    )(
        embedded, previous_out[0], top_grad, grad_out[0], saved_input[0], sqkv, norm_gain[0], wq, out_weight[0],
        modality[0], documents[0],
    )
    return fwd[None], bwd[None]


def solution(mesh):
    placed = (
        P("tp", None),
        P("section", "tp", None),
        P("tp", None),
        P("section", "tp", None),
        P("section", "tp", None),
        P("section", None, None, "tp"),
        P("section", None, None),
        P("section", None, None, None, "tp"),
        P("section", None, "tp", None),
        P("section", None, None),
        P("section", None, None),
    )
    return jax.shard_map(
        body,
        mesh=mesh,
        in_specs=placed,
        out_specs=(P("section", "tp", None), P("section", "tp", None)),
        check_vma=False,
    )
```

```python
import functools
import math

import jax
import jax.numpy as jnp
from jax import lax
from jax.experimental import pallas as pl
from jax.experimental.pallas import tpu as pltpu
from jax.sharding import PartitionSpec as P

EPSILON = 1e-05
HEAD_DIM = 128
MESH = pl.DeviceIdType.MESH
BF = jnp.bfloat16
F32 = jnp.float32
LATE = 8
QB = 256


def nt(x, y):
    return lax.dot_general(x, y, (((1,), (1,)), ((), ())), preferred_element_type=F32)


def tn(x, y):
    return lax.dot_general(x, y, (((0,), (0,)), ((), ())), preferred_element_type=F32)


def nn(x, y):
    return jnp.dot(x, y, preferred_element_type=F32)


class Sems:
    def __init__(self, send, recv):
        self.send, self.recv, self.count, self.open = send, recv, 0, []

    def copy(self, src, dst, peer):
        i = self.count
        self.count += 1
        c = pltpu.make_async_remote_copy(
            src_ref=src, dst_ref=dst, send_sem=self.send.at[i], recv_sem=self.recv.at[i],
            device_id=peer, device_id_type=MESH,
        )
        c.start()
        self.open.append(c)
        return i

    def copy_either(self, cond, src, other, dst, peer):
        i = self.count
        self.count += 1
        yes, no = (
            pltpu.make_async_remote_copy(
                src_ref=x, dst_ref=dst, send_sem=self.send.at[i], recv_sem=self.recv.at[i],
                device_id=peer, device_id_type=MESH,
            )
            for x in (src, other)
        )
        pl.when(cond)(yes.start)
        pl.when(jnp.logical_not(cond))(no.start)
        self.open.append(no)
        return i

    def landed(self, ref, i, peer):
        pltpu.make_async_remote_copy(
            src_ref=ref, dst_ref=ref, send_sem=self.send.at[i], recv_sem=self.recv.at[i],
            device_id=peer, device_id_type=MESH,
        ).wait_recv()

    def drain(self):
        for c in self.open:
            c.wait_send()


N_SEMS = 144
N_LOCAL = 16


def kernel(
    emb, prev, topg, gout, sin, sqkv, gain, wq, wo, mod, doc,
    fout, bout,
    w1, wor, inp, embv, ups, topv, sinv, qkvv, ag, proj, attg, op, oz1, oz2, fo, fa,
    u, gap, gar, gat, pb, ds, dkv, gr, g, gx1, gx2, sx, gz1, gz2, lt, dt, acc,
    ssem, rsem, lsem,
):
    s = lax.axis_index("section")
    t = lax.axis_index("tp")
    n_sec = lax.axis_size("section")
    a, b = t % 4, t // 4
    aR, aL, aO = (a + 1) % 4, (a + 3) % 4, (a + 2) % 4
    bR, bL, bO = (b + 1) % 4, (b + 3) % 4, (b + 2) % 4
    XR, XL, XO = (s, 4 * b + aR), (s, 4 * b + aL), (s, 4 * b + aO)
    ZR, ZL = (s, 4 * bR + a), (s, 4 * bL + a)
    after, before = (s + 1) % n_sec, (s + n_sec - 1) % n_sec
    SR, SL = (after, t), (before, t)
    column = (a, aR, aL, aO)
    SRs, SLs = [(after, 4 * b + k) for k in column], [(before, 4 * b + k) for k in column]
    rows = inp.shape[0]
    width = inp.shape[1]
    half = width // 2
    quarter = width // 4
    length = ag.shape[0] * rows
    chunk = 4 * rows
    scale = 1.0 / math.sqrt(HEAD_DIM)

    bar = pltpu.get_barrier_semaphore()
    for peer in (*SRs, *SLs, XR, XL, XO, ZR, ZL):
        pl.semaphore_signal(bar, inc=1, device_id=peer, device_id_type=MESH)
    pl.semaphore_wait(bar, 13)

    q = Sems(ssem, rsem)
    local = []

    def fetch(src, dst):
        c = pltpu.make_async_copy(src, dst, lsem.at[len(local)])
        c.start()
        local.append(c)
        return c

    mine_rows = pl.ds(pl.multiple_of(a * rows, rows), rows)
    i_up = []
    for peer, k in zip(SLs, column):
        cols = pl.ds(pl.multiple_of(k * quarter, quarter), quarter)
        i_up.append(q.copy_either(s == 0, topg.at[:, cols], gout.at[:, cols], u.at[b, mine_rows, :], peer))
    i_shift_f = q.copy(prev, inp, SR)

    def regroup(m):
        mine = fetch(wo.at[m, :, pl.ds(pl.multiple_of(a * quarter, quarter), quarter)], wor.at[m, a])
        ids = []
        for peer, col in ((XR, aR), (XL, aL), (XO, aO)):
            src = wo.at[m, :, pl.ds(pl.multiple_of(col * quarter, quarter), quarter)]
            ids.append(q.copy(src, wor.at[m, a], peer))
        return mine, ids

    f_qkv = fetch(sqkv, qkvv)
    f_emb = fetch(emb, embv)
    f_top = fetch(topg, topv)
    f_sin = fetch(sin, sinv)
    wo0 = regroup(0)
    wo1 = regroup(1)
    f_w1 = [
        fetch(wq.at[m, j], w1.at[:, pl.ds(m * 384 + j * 128, 128)]) for m in range(2) for j in range(3)
    ]

    for k in range(2):
        lt[k] = jnp.broadcast_to(mod[k : k + 1, :].astype(F32), (128, length)).T
        dt[k] = jnp.broadcast_to(doc[k : k + 1, :].astype(F32), (128, length)).T

    def softmax_block(qb, kb, which, i):
        n = (i + 1) * QB
        sc = nt(qb, kb) * scale
        qpos = lax.broadcasted_iota(jnp.int32, (QB, n), 0) + i * QB
        kpos = lax.broadcasted_iota(jnp.int32, (QB, n), 1)
        dq = dt[which, i * QB : (i + 1) * QB, 0:1]
        dk = doc[which : which + 1, 0:n].astype(F32)
        sc = jnp.where((kpos <= qpos) & (dq == dk), sc, -jnp.inf)
        e = jnp.exp(sc - jnp.max(sc, axis=-1, keepdims=True))
        return e / jnp.sum(e, axis=-1, keepdims=True)

    n_blocks = length // QB

    def saved_probs():
        for i in range(n_blocks):
            pb[i * QB : (i + 1) * QB, 0 : (i + 1) * QB] = softmax_block(
                qkvv[0, i * QB : (i + 1) * QB, :], qkvv[1, 0 : (i + 1) * QB, :], 1, i
            )

    f_qkv.wait()
    f_emb.wait()
    f_top.wait()

    q.landed(inp, i_shift_f, SL)

    def norm_rows(r, _):
        r0 = pl.multiple_of(r * 16, 16)
        x = jnp.where(s == 0, embv[pl.ds(r0, 16), :], inp[pl.ds(r0, 16), :])
        inp[pl.ds(r0, 16), :] = x
        x = x.astype(F32)
        inv = lax.rsqrt(jnp.mean(x * x, axis=-1, keepdims=True) + EPSILON)
        lab = lt[0, pl.ds(pl.multiple_of(t * rows + r0, 16), 16), 0:1]
        gn = jnp.where(lab == 0.0, gain[0:1, :], gain[1:2, :])
        ag[t, pl.ds(r0, 16), :] = (x * inv * gn).astype(BF)
        return 0

    lax.fori_loop(0, rows // 16, norm_rows, 0)
    late = width // LATE
    early = width - late
    h0, h1 = pl.ds(0, half), pl.ds(half, half)
    qh0, qh1 = pl.ds(0, quarter // 2), pl.ds(quarter // 2, quarter // 2)
    ea = pl.ds(0, early)
    e0, e1 = pl.ds(0, early // 2), pl.ds(early // 2, early // 2)
    la = pl.ds(early, late)
    l0, l1 = pl.ds(early, late // 2), pl.ds(early + late // 2, late // 2)
    full = pl.ds(0, width)
    parts = {"B": (full, h0, h1), "L": (ea, e0, e1), "R": (ea, e0, e1), "O": (ea, e0, e1)}
    slotL, slotR, slotO = 4 * bL + a, 4 * bR + a, 4 * bO + a
    quad, quadL, quadR, quadO = (pl.ds(pl.multiple_of(4 * bb, 4), 4) for bb in (b, bL, bR, bO))

    def same(ref, peer):
        return q.copy(ref, ref, peer)

    i_nx, i_nxf = {}, {}

    def spread_x(key, slot):
        c = parts[key][0]
        i_nx[key] = same(ag.at[slot, :, c], XR), same(ag.at[slot, :, c], XL)

    def forward_x(key, bb):
        sl, sr = 4 * bb + aL, 4 * bb + aR
        c, c0, c1 = parts[key]
        q.landed(ag.at[sl, :, c], i_nx[key][0], XL)
        i0 = same(ag.at[sl, :, c0], XR)
        q.landed(ag.at[sr, :, c], i_nx[key][1], XR)
        i1 = same(ag.at[sr, :, c1], XL)
        i_nxf[key] = i0, i1

    def complete_x(key, bb):
        so = 4 * bb + aO
        c, c0, c1 = parts[key]
        q.landed(ag.at[so, :, c0], i_nxf[key][0], XL)
        q.landed(ag.at[so, :, c1], i_nxf[key][1], XR)

    KT = 512

    def project(bb):
        acc[...] = jnp.zeros_like(acc)

        def step(k, _):
            k0 = pl.ds(pl.multiple_of(k * KT, KT), KT)
            x = ag[pl.ds(4 * bb, 4), :, k0].reshape(chunk, KT)
            acc[...] += nn(x, w1[k0, :])
            return 0

        lax.fori_loop(0, width // KT, step, 0)
        r = pl.ds(pl.multiple_of(bb * chunk, chunk), chunk)
        lab = lt[0, r, 0:1]
        proj[r, :] = jnp.where(lab == 0.0, acc[:, 0:384], acc[:, 384:768]).astype(BF)

    i_nz = same(ag.at[t, :, ea], ZR), same(ag.at[t, :, ea], ZL)
    spread_x("B", t)
    saved_probs()

    q.landed(ag.at[slotL, :, ea], i_nz[0], ZL)
    i_nzf0 = same(ag.at[slotL, :, e0], ZR)
    spread_x("L", slotL)
    q.landed(ag.at[slotR, :, ea], i_nz[1], ZR)
    i_nzf1 = same(ag.at[slotR, :, e1], ZL)
    spread_x("R", slotR)

    for i, peer, src_a in zip(i_up, SRs, column):
        q.landed(u.at[b, pl.ds(pl.multiple_of(src_a * rows, rows), rows), :], i, peer)
    i_uz = same(u.at[b], ZR), same(u.at[b], ZL)
    forward_x("B", b)

    for mine, ids in (wo0, wo1):
        mine.wait()
    for m, (mine, ids) in enumerate((wo0, wo1)):
        for i, peer, src_a in zip(ids, (XL, XR, XO), (aL, aR, aO)):
            q.landed(wor.at[m, src_a], i, peer)

    def grad_att(bb):
        r = pl.ds(pl.multiple_of(bb * chunk, chunk), chunk)
        lab = lt[1, r, 0:1]
        x = u[bb]
        for hp in range(2):
            y0 = nt(x, wor[0, 2 * hp : 2 * hp + 2].reshape(256, quarter))
            y1 = nt(x, wor[1, 2 * hp : 2 * hp + 2].reshape(256, quarter))
            y = jnp.where(lab == 0.0, y0, y1).astype(BF)
            gap[2 * hp, r, :] = y[:, 0:128]
            gap[2 * hp + 1, r, :] = y[:, 128:256]

    grad_att(b)
    q.landed(ag.at[slotO, :, e0], i_nzf0, ZL)
    q.landed(ag.at[slotO, :, e1], i_nzf1, ZR)
    spread_x("O", slotO)
    forward_x("L", bL)
    forward_x("R", bR)
    q.landed(u.at[bL], i_uz[0], ZL)
    i_uzf0 = same(u.at[bL, :, qh0], ZR)
    q.landed(u.at[bR], i_uz[1], ZR)
    i_uzf1 = same(u.at[bR, :, qh1], ZL)
    complete_x("B", b)
    i_tz = same(ag.at[quad, :, la], ZR), same(ag.at[quad, :, la], ZL)
    grad_att(bL)
    grad_att(bR)
    for c in f_w1:
        c.wait()
    project(b)
    forward_x("O", bO)
    q.landed(u.at[bO, :, qh0], i_uzf0, ZL)
    q.landed(u.at[bO, :, qh1], i_uzf1, ZR)
    grad_att(bO)
    i_ga = [q.copy(gap.at[k], gar.at[a], peer) for peer, k in ((XR, aR), (XL, aL), (XO, aO))]
    q.landed(ag.at[quadL, :, la], i_tz[0], ZL)
    i_tzf0 = same(ag.at[quadL, :, l0], ZR)
    q.landed(ag.at[quadR, :, la], i_tz[1], ZR)
    i_tzf1 = same(ag.at[quadR, :, l1], ZL)
    i_shift_b = q.copy(gout, ups, SL)
    complete_x("L", bL)
    project(bL)
    complete_x("R", bR)
    project(bR)

    complete_x("O", bO)
    q.landed(ag.at[quadO, :, l0], i_tzf0, ZL)
    q.landed(ag.at[quadO, :, l1], i_tzf1, ZR)
    project(bO)

    for i in range(n_blocks):
        r = slice(i * QB, (i + 1) * QB)
        n = (i + 1) * QB
        p = softmax_block(proj[r, 0:128], proj[0:n, 128:256], 0, i).astype(BF)
        attg[a, r, :] = nn(p, proj[0:n, 256:384]).astype(BF)
    i_at = [q.copy(attg.at[a], attg.at[a], peer) for peer in (XR, XL, XO)]

    for i, peer, src_a in zip(i_ga, (XL, XR, XO), (aL, aR, aO)):
        q.landed(gar.at[src_a], i, peer)

    def sum_ga(r, _):
        rr = pl.ds(pl.multiple_of(r * 64, 64), 64)
        total = gap[a, rr, :].astype(F32) + gar[aL, rr, :].astype(F32)
        total += gar[aR, rr, :].astype(F32) + gar[aO, rr, :].astype(F32)
        gat[rr, :] = total.astype(BF)
        return 0

    lax.fori_loop(0, length // 64, sum_ga, 0)

    for i in range(n_blocks):
        r = slice(i * QB, (i + 1) * QB)
        n = (i + 1) * QB
        p = pb[r, 0:n]
        gp = nt(gat[r, :], qkvv[2, 0:n, :])
        delta = jnp.sum(p * gp, axis=-1, keepdims=True)
        d = (p * (gp - delta) * scale).astype(BF)
        ds[r, 0:n] = d
        dq = nn(d, qkvv[1, 0:n, :]).astype(BF)
        lab = lt[1, r, 0:1]
        zero = jnp.zeros_like(dq)
        gr[r, 0:128] = jnp.where(lab == 0.0, dq, zero)
        gr[r, 384:512] = jnp.where(lab == 0.0, zero, dq)
    for j in range(n_blocks):
        cols = slice(j * QB, (j + 1) * QB)
        dk = jnp.zeros((QB, HEAD_DIM), F32)
        dv = jnp.zeros((QB, HEAD_DIM), F32)
        for i in range(j, n_blocks):
            r = slice(i * QB, (i + 1) * QB)
            dk += tn(ds[r, cols], qkvv[0, r, :])
            dv += tn(pb[r, cols].astype(BF), gat[r, :])
        lab = lt[1, cols, 0:1]
        zero = jnp.zeros((QB, HEAD_DIM), BF)
        gr[cols, 128:256] = jnp.where(lab == 0.0, dk.astype(BF), zero)
        gr[cols, 512:640] = jnp.where(lab == 0.0, zero, dk.astype(BF))
        gr[cols, 256:384] = jnp.where(lab == 0.0, dv.astype(BF), zero)
        gr[cols, 640:768] = jnp.where(lab == 0.0, zero, dv.astype(BF))

    def grad_in(bb, c0, w):
        r = pl.ds(pl.multiple_of(bb * chunk, chunk), chunk)

        def step(k, _):
            k0 = pl.ds(pl.multiple_of(c0 + k * KT, KT), KT)
            y = nt(gr[r, :], w1[k0, :]).astype(BF)
            g[pl.ds(4 * bb, 4), :, k0] = y.reshape(4, rows, KT)
            return 0

        lax.fori_loop(0, w // KT, step, 0)

    units = [
        [(bO, 0, 0, half)],
        [(bO, 0, half, half)],
        [(bR, 1, 0, half)],
        [(bL, 2, half, half)],
        [(bR, 1, half, half)],
        [(bL, 2, 0, half)],
        [(b, 3, 0, half)],
        [(b, 3, half, half)],
    ]
    i_gx = {}

    def gx_send(k):
        for p, (bb, role, c0, w) in enumerate(units[k]):
            grad_in(bb, c0, w)
        for p, (bb, role, c0, w) in enumerate(units[k]):
            lo, hi = pl.ds(c0, w // 2), pl.ds(c0 + w // 2, w // 2)
            o, l, r = 4 * bb + aO, 4 * bb + aL, 4 * bb + aR
            i_gx[k, p] = [
                q.copy(g.at[o, :, lo], gx1.at[role, 0, :, pl.ds(c0 // 2, w // 2)], XL),
                q.copy(g.at[o, :, hi], gx1.at[role, 1, :, pl.ds(c0 // 2, w // 2)], XR),
                q.copy(g.at[l, :, hi], gx2.at[role, 0, :, hi], XL),
                q.copy(g.at[r, :, lo], gx2.at[role, 1, :, lo], XR),
            ]

    def gx_pass(k):
        for p, (bb, role, c0, w) in enumerate(units[k]):
            lo, hi = pl.ds(c0, w // 2), pl.ds(c0 + w // 2, w // 2)
            mid = pl.ds(c0 // 2, w // 2)
            l, r = 4 * bb + aL, 4 * bb + aR
            ids = i_gx[k, p]
            q.landed(gx1.at[role, 0, :, mid], ids[0], XR)
            g[l, :, lo] = (g[l, :, lo].astype(F32) + gx1[role, 0, :, mid].astype(F32)).astype(BF)
            i0 = q.copy(g.at[l, :, lo], gx2.at[role, 0, :, lo], XL)
            q.landed(gx1.at[role, 1, :, mid], ids[1], XL)
            g[r, :, hi] = (g[r, :, hi].astype(F32) + gx1[role, 1, :, mid].astype(F32)).astype(BF)
            i1 = q.copy(g.at[r, :, hi], gx2.at[role, 1, :, hi], XR)
            ids += [i0, i1]

    def gx_sum(k, more=None):
        for p, (bb, role, c0, w) in enumerate(units[k]):
            lo, hi = pl.ds(c0, w // 2), pl.ds(c0 + w // 2, w // 2)
            ids = i_gx[k, p]
            q.landed(gx2.at[role, 0, :, hi], ids[2], XR)
            q.landed(gx2.at[role, 1, :, lo], ids[3], XL)
            q.landed(gx2.at[role, 0, :, lo], ids[4], XR)
            q.landed(gx2.at[role, 1, :, hi], ids[5], XL)
            own = 4 * bb + a

            def step(c, _):
                cc = pl.ds(pl.multiple_of(c0 + c * KT, KT), KT)
                total = g[own, :, cc].astype(F32) + gx2[role, 0, :, cc].astype(F32) + gx2[role, 1, :, cc].astype(F32)
                if more is not None:
                    total += gz1[more[p], :, pl.ds(pl.multiple_of(c * KT, KT), KT)].astype(F32)
                sx[role, :, cc] = total.astype(BF)
                return 0

            lax.fori_loop(0, w // KT, step, 0)

    gx_send(0)
    gx_send(1)
    gx_send(2)

    def out_proj(bb, k):
        r = pl.ds(pl.multiple_of(bb * chunk, chunk), chunk)
        lab = lt[0, r, 0:1]
        heads = [attg[h, r, :] for h in range(4)]
        zero = jnp.zeros((chunk, HEAD_DIM), BF)
        x = jnp.concatenate(
            [jnp.where(lab == 0.0, h, zero) for h in heads] + [jnp.where(lab == 0.0, zero, h) for h in heads], axis=1
        )
        for c in range(2):
            y = wor[:, :, :, c * 512 : (c + 1) * 512].reshape(1024, 512)
            op[k, :, c * 512 : (c + 1) * 512] = nn(x, y).astype(BF)

    for i, peer, src_a in zip(i_at, (XL, XR, XO), (aL, aR, aO)):
        q.landed(attg.at[src_a], i, peer)
    out_proj(bO, 0)
    i_oz = [q.copy(op.at[0, :, qh0], oz1.at[0], ZL), q.copy(op.at[0, :, qh1], oz1.at[1], ZR)]
    out_proj(bR, 1)
    i_oz.append(q.copy(op.at[1, :, qh0], oz2.at[1, :, qh0], ZR))
    out_proj(bL, 2)
    i_oz.append(q.copy(op.at[2, :, qh1], oz2.at[0, :, qh1], ZL))
    gx_pass(0)
    gx_send(3)
    out_proj(b, 3)
    gx_pass(1)
    gx_sum(0)
    i_gz1 = [q.copy(sx.at[0, :, h0], gz1.at[0], ZL)]
    gx_send(4)
    gx_pass(2)
    gx_sum(1)
    i_gz1.append(q.copy(sx.at[0, :, h1], gz1.at[1], ZR))
    gx_send(5)
    q.landed(oz1.at[0], i_oz[0], ZR)
    op[2, :, qh0] = (op[2, :, qh0].astype(F32) + oz1[0].astype(F32)).astype(BF)
    i_oz.append(q.copy(op.at[2, :, qh0], oz2.at[0, :, qh0], ZL))
    q.landed(oz1.at[1], i_oz[1], ZL)
    op[1, :, qh1] = (op[1, :, qh1].astype(F32) + oz1[1].astype(F32)).astype(BF)
    i_oz.append(q.copy(op.at[1, :, qh1], oz2.at[1, :, qh1], ZR))
    gx_pass(3)
    gx_sum(2)
    i_gz2 = [q.copy(sx.at[1, :, h0], gz2.at[1, :, h0], ZR)]
    gx_send(6)
    gx_pass(4)
    gx_sum(3)
    i_gz2.append(q.copy(sx.at[2, :, h1], gz2.at[0, :, h1], ZL))
    gx_send(7)
    gx_pass(5)
    gx_pass(6)
    q.landed(gz1.at[1], i_gz1[1], ZL)
    gx_sum(4, (1,))
    i_gz2.append(q.copy(sx.at[1, :, h1], gz2.at[1, :, h1], ZR))
    gx_pass(7)
    q.landed(gz1.at[0], i_gz1[0], ZR)
    gx_sum(5, (0,))
    i_gz2.append(q.copy(sx.at[2, :, h0], gz2.at[0, :, h0], ZL))

    q.landed(oz2.at[1, :, qh0], i_oz[2], ZL)
    q.landed(oz2.at[0, :, qh1], i_oz[3], ZR)
    q.landed(oz2.at[0, :, qh0], i_oz[4], ZR)
    q.landed(oz2.at[1, :, qh1], i_oz[5], ZL)

    def sum_out(k, _):
        rr = pl.ds(pl.multiple_of(k * rows, rows), rows)
        total = op[3, rr, :].astype(F32) + oz2[0, rr, :].astype(F32) + oz2[1, rr, :].astype(F32)
        fo[k] = total.astype(BF)
        return 0

    lax.fori_loop(0, 4, sum_out, 0)
    i_fa = [q.copy(fo.at[k], fa.at[a], peer) for peer, k in ((XR, aR), (XL, aL), (XO, aO))]
    fa[a] = fo[a]

    f_sin.wait()
    gx_sum(6)
    gx_sum(7)

    for i, peer, src_a in zip(i_fa, (XL, XR, XO), (aL, aR, aO)):
        q.landed(fa.at[src_a], i, peer)
    for k in range(4):
        cols = slice(k * quarter, (k + 1) * quarter)
        fout[:, cols] = (inp[:, cols].astype(F32) + fa[k].astype(F32)).astype(BF)

    q.landed(ups, i_shift_b, SR)
    q.landed(gz2.at[1, :, h0], i_gz2[0], ZL)
    q.landed(gz2.at[0, :, h1], i_gz2[1], ZR)
    q.landed(gz2.at[1, :, h1], i_gz2[2], ZL)
    q.landed(gz2.at[0, :, h0], i_gz2[3], ZR)

    def back_rows(r, _):
        rr = pl.ds(pl.multiple_of(r * 16, 16), 16)
        total = sx[3, rr, :].astype(F32) + gz2[0, rr, :].astype(F32) + gz2[1, rr, :].astype(F32)
        lab = lt[1, pl.ds(pl.multiple_of(t * rows + r * 16, 16), 16), 0:1]
        scaled = total * jnp.where(lab == 0.0, gain[0:1, :], gain[1:2, :])
        x = sinv[rr, :].astype(F32)
        inv = lax.rsqrt(jnp.mean(x * x, axis=-1, keepdims=True) + EPSILON)
        corr = jnp.mean(scaled * x, axis=-1, keepdims=True)
        up = jnp.where(s == n_sec - 1, topv[rr, :], ups[rr, :]).astype(F32)
        bout[rr, :] = (up + inv * scaled - x * inv * inv * inv * corr).astype(BF)
        return 0

    lax.fori_loop(0, rows // 16, back_rows, 0)
    q.drain()


def body(
    embedded, previous_out, top_grad, grad_out, saved_input, saved_qkv, norm_gain, qkv_weight, out_weight,
    modality, documents,
):
    rows, width = embedded.shape
    length = saved_qkv.shape[1]
    blocks = length // rows
    quarter = width // 4
    wq = jnp.transpose(qkv_weight[0], (0, 2, 1, 3))
    sqkv = jnp.transpose(saved_qkv[0], (1, 0, 2))
    vm = pl.BlockSpec(memory_space=pltpu.VMEM)
    hb = pl.BlockSpec(memory_space=pl.ANY)
    v = pltpu.VMEM
    out = jax.ShapeDtypeStruct((rows, width), BF)
    chunk = 4 * rows
    fwd, bwd = pl.pallas_call(
        kernel,
        out_shape=(out, out),
        in_specs=[hb, hb, hb, hb, hb, hb, vm, hb, hb, vm, vm],
        out_specs=(vm, vm),
        scratch_shapes=[
            v((width, 768), BF),
            v((2, 4, 128, quarter), BF),
            v((rows, width), BF),
            v((rows, width), BF),
            v((rows, width), BF),
            v((rows, width), BF),
            v((rows, width), BF),
            v((3, length, HEAD_DIM), BF),
            v((blocks, rows, width), BF),
            v((length, 384), BF),
            v((4, length, HEAD_DIM), BF),
            v((4, chunk, quarter), BF),
            v((2, chunk, quarter // 2), BF),
            v((2, chunk, quarter), BF),
            v((4, rows, quarter), BF),
            v((4, rows, quarter), BF),
            v((4, chunk, quarter), BF),
            v((4, length, HEAD_DIM), BF),
            v((4, length, HEAD_DIM), BF),
            v((length, HEAD_DIM), BF),
            v((length, length), F32),
            v((length, length), BF),
            v((8, 128), F32),
            v((length, 768), BF),
            v((blocks, rows, width), BF),
            v((4, 2, rows, width // 2), BF),
            v((4, 2, rows, width), BF),
            v((4, rows, width), BF),
            v((2, rows, width // 2), BF),
            v((2, rows, width), BF),
            v((2, length, 128), F32),
            v((2, length, 128), F32),
            v((chunk, 768), F32),
            pltpu.SemaphoreType.DMA((N_SEMS,)),
            pltpu.SemaphoreType.DMA((N_SEMS,)),
            pltpu.SemaphoreType.DMA((N_LOCAL,)),
        ],
        compiler_params=pltpu.CompilerParams(
            collective_id=0, has_side_effects=True, vmem_limit_bytes=62 * 1024 * 1024
        ),
        name="relay",
    )(
        embedded, previous_out[0], top_grad, grad_out[0], saved_input[0], sqkv, norm_gain[0], wq, out_weight[0],
        modality[0], documents[0],
    )
    return fwd[None], bwd[None]


def solution(mesh):
    placed = (
        P("tp", None),
        P("section", "tp", None),
        P("tp", None),
        P("section", "tp", None),
        P("section", "tp", None),
        P("section", None, None, "tp"),
        P("section", None, None),
        P("section", None, None, None, "tp"),
        P("section", None, "tp", None),
        P("section", None, None),
        P("section", None, None),
    )
    return jax.shard_map(
        body,
        mesh=mesh,
        in_specs=placed,
        out_specs=(P("section", "tp", None), P("section", "tp", None)),
        check_vma=False,
    )
```

```python
import functools
import math

import jax
import jax.numpy as jnp
from jax import lax
from jax.experimental import pallas as pl
from jax.experimental.pallas import tpu as pltpu
from jax.sharding import PartitionSpec as P

EPSILON = 1e-05
HEAD_DIM = 128
MESH = pl.DeviceIdType.MESH
BF = jnp.bfloat16
F32 = jnp.float32
LATE = 8
QB = 256


def nt(x, y):
    return lax.dot_general(x, y, (((1,), (1,)), ((), ())), preferred_element_type=F32)


def tn(x, y):
    return lax.dot_general(x, y, (((0,), (0,)), ((), ())), preferred_element_type=F32)


def nn(x, y):
    return jnp.dot(x, y, preferred_element_type=F32)


class Sems:
    def __init__(self, send, recv):
        self.send, self.recv, self.count, self.open = send, recv, 0, []

    def copy(self, src, dst, peer):
        i = self.count
        self.count += 1
        c = pltpu.make_async_remote_copy(
            src_ref=src, dst_ref=dst, send_sem=self.send.at[i], recv_sem=self.recv.at[i],
            device_id=peer, device_id_type=MESH,
        )
        c.start()
        self.open.append(c)
        return i

    def copy_either(self, cond, src, other, dst, peer):
        i = self.count
        self.count += 1
        yes, no = (
            pltpu.make_async_remote_copy(
                src_ref=x, dst_ref=dst, send_sem=self.send.at[i], recv_sem=self.recv.at[i],
                device_id=peer, device_id_type=MESH,
            )
            for x in (src, other)
        )
        pl.when(cond)(yes.start)
        pl.when(jnp.logical_not(cond))(no.start)
        self.open.append(no)
        return i

    def landed(self, ref, i, peer):
        pltpu.make_async_remote_copy(
            src_ref=ref, dst_ref=ref, send_sem=self.send.at[i], recv_sem=self.recv.at[i],
            device_id=peer, device_id_type=MESH,
        ).wait_recv()

    def drain(self):
        for c in self.open:
            c.wait_send()


N_SEMS = 144
N_LOCAL = 16


def kernel(
    emb, prev, topg, gout, sin, sqkv, gain_in, wq, wo, mod_in, doc_in,
    fout, bout,
    gain, mod, doc, w1, wor, inp, embv, ups, topv, sinv, qkvv, ag, proj, attg, op, oz1, oz2, fo, fa,
    u, gap, gar, gat, pb, ds, dkv, gr, g, gx1, gx2, sx, gz1, gz2, lt, dt, acc,
    ssem, rsem, lsem,
):
    s = lax.axis_index("section")
    t = lax.axis_index("tp")
    n_sec = lax.axis_size("section")
    a, b = t % 4, t // 4
    aR, aL, aO = (a + 1) % 4, (a + 3) % 4, (a + 2) % 4
    bR, bL, bO = (b + 1) % 4, (b + 3) % 4, (b + 2) % 4
    XR, XL, XO = (s, 4 * b + aR), (s, 4 * b + aL), (s, 4 * b + aO)
    ZR, ZL = (s, 4 * bR + a), (s, 4 * bL + a)
    after, before = (s + 1) % n_sec, (s + n_sec - 1) % n_sec
    SR, SL = (after, t), (before, t)
    column = (a, aR, aL, aO)
    SRs, SLs = [(after, 4 * b + k) for k in column], [(before, 4 * b + k) for k in column]
    rows = inp.shape[0]
    width = inp.shape[1]
    half = width // 2
    quarter = width // 4
    length = ag.shape[0] * rows
    chunk = 4 * rows
    scale = 1.0 / math.sqrt(HEAD_DIM)

    local = []

    def fetch(src, dst):
        c = pltpu.make_async_copy(src, dst, lsem.at[len(local)])
        c.start()
        local.append(c)
        return c

    f_small = [fetch(mod_in, mod), fetch(doc_in, doc), fetch(gain_in, gain)]
    bar = pltpu.get_barrier_semaphore()
    for peer in (*SRs, *SLs, XR, XL, XO, ZR, ZL):
        pl.semaphore_signal(bar, inc=1, device_id=peer, device_id_type=MESH)
    pl.semaphore_wait(bar, 13)

    q = Sems(ssem, rsem)

    mine_rows = pl.ds(pl.multiple_of(a * rows, rows), rows)
    i_up = []
    for peer, k in zip(SLs, column):
        cols = pl.ds(pl.multiple_of(k * quarter, quarter), quarter)
        i_up.append(q.copy_either(s == 0, topg.at[:, cols], gout.at[:, cols], u.at[b, mine_rows, :], peer))
    i_shift_f = q.copy(prev, inp, SR)

    def regroup(m):
        mine = fetch(wo.at[m, :, pl.ds(pl.multiple_of(a * quarter, quarter), quarter)], wor.at[m, a])
        ids = []
        for peer, col in ((XR, aR), (XL, aL), (XO, aO)):
            src = wo.at[m, :, pl.ds(pl.multiple_of(col * quarter, quarter), quarter)]
            ids.append(q.copy(src, wor.at[m, a], peer))
        return mine, ids

    f_qkv = fetch(sqkv, qkvv)
    f_emb = fetch(emb, embv)
    f_top = fetch(topg, topv)
    f_sin = fetch(sin, sinv)
    wo0 = regroup(0)
    wo1 = regroup(1)
    f_w1 = [
        fetch(wq.at[m, j], w1.at[:, pl.ds(m * 384 + j * 128, 128)]) for m in range(2) for j in range(3)
    ]

    for c in f_small:
        c.wait()
    for k in range(2):
        lt[k] = jnp.broadcast_to(mod[k : k + 1, :].astype(F32), (128, length)).T
        dt[k] = jnp.broadcast_to(doc[k : k + 1, :].astype(F32), (128, length)).T

    def softmax_block(qb, kb, which, i):
        n = (i + 1) * QB
        sc = nt(qb, kb) * scale
        qpos = lax.broadcasted_iota(jnp.int32, (QB, n), 0) + i * QB
        kpos = lax.broadcasted_iota(jnp.int32, (QB, n), 1)
        dq = dt[which, i * QB : (i + 1) * QB, 0:1]
        dk = doc[which : which + 1, 0:n].astype(F32)
        sc = jnp.where((kpos <= qpos) & (dq == dk), sc, -jnp.inf)
        e = jnp.exp(sc - jnp.max(sc, axis=-1, keepdims=True))
        return e / jnp.sum(e, axis=-1, keepdims=True)

    n_blocks = length // QB

    def saved_probs():
        for i in range(n_blocks):
            pb[i * QB : (i + 1) * QB, 0 : (i + 1) * QB] = softmax_block(
                qkvv[0, i * QB : (i + 1) * QB, :], qkvv[1, 0 : (i + 1) * QB, :], 1, i
            )

    f_qkv.wait()
    f_emb.wait()
    f_top.wait()

    q.landed(inp, i_shift_f, SL)

    def norm_rows(r, _):
        r0 = pl.multiple_of(r * 16, 16)
        x = jnp.where(s == 0, embv[pl.ds(r0, 16), :], inp[pl.ds(r0, 16), :])
        inp[pl.ds(r0, 16), :] = x
        x = x.astype(F32)
        inv = lax.rsqrt(jnp.mean(x * x, axis=-1, keepdims=True) + EPSILON)
        lab = lt[0, pl.ds(pl.multiple_of(t * rows + r0, 16), 16), 0:1]
        gn = jnp.where(lab == 0.0, gain[0:1, :], gain[1:2, :])
        ag[t, pl.ds(r0, 16), :] = (x * inv * gn).astype(BF)
        return 0

    lax.fori_loop(0, rows // 16, norm_rows, 0)
    late = width // LATE
    early = width - late
    h0, h1 = pl.ds(0, half), pl.ds(half, half)
    qh0, qh1 = pl.ds(0, quarter // 2), pl.ds(quarter // 2, quarter // 2)
    ea = pl.ds(0, early)
    e0, e1 = pl.ds(0, early // 2), pl.ds(early // 2, early // 2)
    la = pl.ds(early, late)
    l0, l1 = pl.ds(early, late // 2), pl.ds(early + late // 2, late // 2)
    full = pl.ds(0, width)
    parts = {"B": (full, h0, h1), "L": (ea, e0, e1), "R": (ea, e0, e1), "O": (ea, e0, e1)}
    slotL, slotR, slotO = 4 * bL + a, 4 * bR + a, 4 * bO + a
    quad, quadL, quadR, quadO = (pl.ds(pl.multiple_of(4 * bb, 4), 4) for bb in (b, bL, bR, bO))

    def same(ref, peer):
        return q.copy(ref, ref, peer)

    i_nx, i_nxf = {}, {}

    def spread_x(key, slot):
        c = parts[key][0]
        i_nx[key] = same(ag.at[slot, :, c], XR), same(ag.at[slot, :, c], XL)

    def forward_x(key, bb):
        sl, sr = 4 * bb + aL, 4 * bb + aR
        c, c0, c1 = parts[key]
        q.landed(ag.at[sl, :, c], i_nx[key][0], XL)
        i0 = same(ag.at[sl, :, c0], XR)
        q.landed(ag.at[sr, :, c], i_nx[key][1], XR)
        i1 = same(ag.at[sr, :, c1], XL)
        i_nxf[key] = i0, i1

    def complete_x(key, bb):
        so = 4 * bb + aO
        c, c0, c1 = parts[key]
        q.landed(ag.at[so, :, c0], i_nxf[key][0], XL)
        q.landed(ag.at[so, :, c1], i_nxf[key][1], XR)

    KT = 512

    def project(bb):
        acc[...] = jnp.zeros_like(acc)

        def step(k, _):
            k0 = pl.ds(pl.multiple_of(k * KT, KT), KT)
            x = ag[pl.ds(4 * bb, 4), :, k0].reshape(chunk, KT)
            acc[...] += nn(x, w1[k0, :])
            return 0

        lax.fori_loop(0, width // KT, step, 0)
        r = pl.ds(pl.multiple_of(bb * chunk, chunk), chunk)
        lab = lt[0, r, 0:1]
        proj[r, :] = jnp.where(lab == 0.0, acc[:, 0:384], acc[:, 384:768]).astype(BF)

    i_nz = same(ag.at[t, :, ea], ZR), same(ag.at[t, :, ea], ZL)
    spread_x("B", t)
    saved_probs()

    q.landed(ag.at[slotL, :, ea], i_nz[0], ZL)
    i_nzf0 = same(ag.at[slotL, :, e0], ZR)
    spread_x("L", slotL)
    q.landed(ag.at[slotR, :, ea], i_nz[1], ZR)
    i_nzf1 = same(ag.at[slotR, :, e1], ZL)
    spread_x("R", slotR)

    for i, peer, src_a in zip(i_up, SRs, column):
        q.landed(u.at[b, pl.ds(pl.multiple_of(src_a * rows, rows), rows), :], i, peer)
    i_uz = same(u.at[b], ZR), same(u.at[b], ZL)
    forward_x("B", b)

    for mine, ids in (wo0, wo1):
        mine.wait()
    for m, (mine, ids) in enumerate((wo0, wo1)):
        for i, peer, src_a in zip(ids, (XL, XR, XO), (aL, aR, aO)):
            q.landed(wor.at[m, src_a], i, peer)

    def grad_att(bb):
        r = pl.ds(pl.multiple_of(bb * chunk, chunk), chunk)
        lab = lt[1, r, 0:1]
        x = u[bb]
        for hp in range(2):
            y0 = nt(x, wor[0, 2 * hp : 2 * hp + 2].reshape(256, quarter))
            y1 = nt(x, wor[1, 2 * hp : 2 * hp + 2].reshape(256, quarter))
            y = jnp.where(lab == 0.0, y0, y1).astype(BF)
            gap[2 * hp, r, :] = y[:, 0:128]
            gap[2 * hp + 1, r, :] = y[:, 128:256]

    grad_att(b)
    q.landed(ag.at[slotO, :, e0], i_nzf0, ZL)
    q.landed(ag.at[slotO, :, e1], i_nzf1, ZR)
    spread_x("O", slotO)
    forward_x("L", bL)
    forward_x("R", bR)
    q.landed(u.at[bL], i_uz[0], ZL)
    i_uzf0 = same(u.at[bL, :, qh0], ZR)
    q.landed(u.at[bR], i_uz[1], ZR)
    i_uzf1 = same(u.at[bR, :, qh1], ZL)
    complete_x("B", b)
    i_tz = same(ag.at[quad, :, la], ZR), same(ag.at[quad, :, la], ZL)
    grad_att(bL)
    grad_att(bR)
    for c in f_w1:
        c.wait()
    project(b)
    forward_x("O", bO)
    q.landed(u.at[bO, :, qh0], i_uzf0, ZL)
    q.landed(u.at[bO, :, qh1], i_uzf1, ZR)
    grad_att(bO)
    i_ga = [q.copy(gap.at[k], gar.at[a], peer) for peer, k in ((XR, aR), (XL, aL), (XO, aO))]
    q.landed(ag.at[quadL, :, la], i_tz[0], ZL)
    i_tzf0 = same(ag.at[quadL, :, l0], ZR)
    q.landed(ag.at[quadR, :, la], i_tz[1], ZR)
    i_tzf1 = same(ag.at[quadR, :, l1], ZL)
    i_shift_b = q.copy(gout, ups, SL)
    complete_x("L", bL)
    project(bL)
    complete_x("R", bR)
    project(bR)

    complete_x("O", bO)
    q.landed(ag.at[quadO, :, l0], i_tzf0, ZL)
    q.landed(ag.at[quadO, :, l1], i_tzf1, ZR)
    project(bO)

    for i in range(n_blocks):
        r = slice(i * QB, (i + 1) * QB)
        n = (i + 1) * QB
        p = softmax_block(proj[r, 0:128], proj[0:n, 128:256], 0, i).astype(BF)
        attg[a, r, :] = nn(p, proj[0:n, 256:384]).astype(BF)
    i_at = [q.copy(attg.at[a], attg.at[a], peer) for peer in (XR, XL, XO)]

    for i, peer, src_a in zip(i_ga, (XL, XR, XO), (aL, aR, aO)):
        q.landed(gar.at[src_a], i, peer)

    def sum_ga(r, _):
        rr = pl.ds(pl.multiple_of(r * 64, 64), 64)
        total = gap[a, rr, :].astype(F32) + gar[aL, rr, :].astype(F32)
        total += gar[aR, rr, :].astype(F32) + gar[aO, rr, :].astype(F32)
        gat[rr, :] = total.astype(BF)
        return 0

    lax.fori_loop(0, length // 64, sum_ga, 0)

    for i in range(n_blocks):
        r = slice(i * QB, (i + 1) * QB)
        n = (i + 1) * QB
        p = pb[r, 0:n]
        gp = nt(gat[r, :], qkvv[2, 0:n, :])
        delta = jnp.sum(p * gp, axis=-1, keepdims=True)
        d = (p * (gp - delta) * scale).astype(BF)
        ds[r, 0:n] = d
        dq = nn(d, qkvv[1, 0:n, :]).astype(BF)
        lab = lt[1, r, 0:1]
        zero = jnp.zeros_like(dq)
        gr[r, 0:128] = jnp.where(lab == 0.0, dq, zero)
        gr[r, 384:512] = jnp.where(lab == 0.0, zero, dq)
    for j in range(n_blocks):
        cols = slice(j * QB, (j + 1) * QB)
        dk = jnp.zeros((QB, HEAD_DIM), F32)
        dv = jnp.zeros((QB, HEAD_DIM), F32)
        for i in range(j, n_blocks):
            r = slice(i * QB, (i + 1) * QB)
            dk += tn(ds[r, cols], qkvv[0, r, :])
            dv += tn(pb[r, cols].astype(BF), gat[r, :])
        lab = lt[1, cols, 0:1]
        zero = jnp.zeros((QB, HEAD_DIM), BF)
        gr[cols, 128:256] = jnp.where(lab == 0.0, dk.astype(BF), zero)
        gr[cols, 512:640] = jnp.where(lab == 0.0, zero, dk.astype(BF))
        gr[cols, 256:384] = jnp.where(lab == 0.0, dv.astype(BF), zero)
        gr[cols, 640:768] = jnp.where(lab == 0.0, zero, dv.astype(BF))

    def grad_in(bb, c0, w):
        r = pl.ds(pl.multiple_of(bb * chunk, chunk), chunk)

        def step(k, _):
            k0 = pl.ds(pl.multiple_of(c0 + k * KT, KT), KT)
            y = nt(gr[r, :], w1[k0, :]).astype(BF)
            g[pl.ds(4 * bb, 4), :, k0] = y.reshape(4, rows, KT)
            return 0

        lax.fori_loop(0, w // KT, step, 0)

    units = [
        [(bO, 0, 0, half)],
        [(bO, 0, half, half)],
        [(bR, 1, 0, half)],
        [(bL, 2, half, half)],
        [(bR, 1, half, half)],
        [(bL, 2, 0, half)],
        [(b, 3, 0, half)],
        [(b, 3, half, half)],
    ]
    i_gx = {}

    def gx_send(k):
        for p, (bb, role, c0, w) in enumerate(units[k]):
            grad_in(bb, c0, w)
        for p, (bb, role, c0, w) in enumerate(units[k]):
            lo, hi = pl.ds(c0, w // 2), pl.ds(c0 + w // 2, w // 2)
            o, l, r = 4 * bb + aO, 4 * bb + aL, 4 * bb + aR
            i_gx[k, p] = [
                q.copy(g.at[o, :, lo], gx1.at[role, 0, :, pl.ds(c0 // 2, w // 2)], XL),
                q.copy(g.at[o, :, hi], gx1.at[role, 1, :, pl.ds(c0 // 2, w // 2)], XR),
                q.copy(g.at[l, :, hi], gx2.at[role, 0, :, hi], XL),
                q.copy(g.at[r, :, lo], gx2.at[role, 1, :, lo], XR),
            ]

    def gx_pass(k):
        for p, (bb, role, c0, w) in enumerate(units[k]):
            lo, hi = pl.ds(c0, w // 2), pl.ds(c0 + w // 2, w // 2)
            mid = pl.ds(c0 // 2, w // 2)
            l, r = 4 * bb + aL, 4 * bb + aR
            ids = i_gx[k, p]
            q.landed(gx1.at[role, 0, :, mid], ids[0], XR)
            g[l, :, lo] = (g[l, :, lo].astype(F32) + gx1[role, 0, :, mid].astype(F32)).astype(BF)
            i0 = q.copy(g.at[l, :, lo], gx2.at[role, 0, :, lo], XL)
            q.landed(gx1.at[role, 1, :, mid], ids[1], XL)
            g[r, :, hi] = (g[r, :, hi].astype(F32) + gx1[role, 1, :, mid].astype(F32)).astype(BF)
            i1 = q.copy(g.at[r, :, hi], gx2.at[role, 1, :, hi], XR)
            ids += [i0, i1]

    def gx_sum(k, more=None):
        for p, (bb, role, c0, w) in enumerate(units[k]):
            lo, hi = pl.ds(c0, w // 2), pl.ds(c0 + w // 2, w // 2)
            ids = i_gx[k, p]
            q.landed(gx2.at[role, 0, :, hi], ids[2], XR)
            q.landed(gx2.at[role, 1, :, lo], ids[3], XL)
            q.landed(gx2.at[role, 0, :, lo], ids[4], XR)
            q.landed(gx2.at[role, 1, :, hi], ids[5], XL)
            own = 4 * bb + a

            def step(c, _):
                cc = pl.ds(pl.multiple_of(c0 + c * KT, KT), KT)
                total = g[own, :, cc].astype(F32) + gx2[role, 0, :, cc].astype(F32) + gx2[role, 1, :, cc].astype(F32)
                if more is not None:
                    total += gz1[more[p], :, pl.ds(pl.multiple_of(c * KT, KT), KT)].astype(F32)
                sx[role, :, cc] = total.astype(BF)
                return 0

            lax.fori_loop(0, w // KT, step, 0)

    gx_send(0)
    gx_send(1)
    gx_send(2)

    def out_proj(bb, k):
        r = pl.ds(pl.multiple_of(bb * chunk, chunk), chunk)
        lab = lt[0, r, 0:1]
        heads = [attg[h, r, :] for h in range(4)]
        zero = jnp.zeros((chunk, HEAD_DIM), BF)
        x = jnp.concatenate(
            [jnp.where(lab == 0.0, h, zero) for h in heads] + [jnp.where(lab == 0.0, zero, h) for h in heads], axis=1
        )
        for c in range(2):
            y = wor[:, :, :, c * 512 : (c + 1) * 512].reshape(1024, 512)
            op[k, :, c * 512 : (c + 1) * 512] = nn(x, y).astype(BF)

    for i, peer, src_a in zip(i_at, (XL, XR, XO), (aL, aR, aO)):
        q.landed(attg.at[src_a], i, peer)
    out_proj(bO, 0)
    i_oz = [q.copy(op.at[0, :, qh0], oz1.at[0], ZL), q.copy(op.at[0, :, qh1], oz1.at[1], ZR)]
    out_proj(bR, 1)
    i_oz.append(q.copy(op.at[1, :, qh0], oz2.at[1, :, qh0], ZR))
    out_proj(bL, 2)
    i_oz.append(q.copy(op.at[2, :, qh1], oz2.at[0, :, qh1], ZL))
    gx_pass(0)
    gx_send(3)
    out_proj(b, 3)
    gx_pass(1)
    gx_sum(0)
    i_gz1 = [q.copy(sx.at[0, :, h0], gz1.at[0], ZL)]
    gx_send(4)
    gx_pass(2)
    gx_sum(1)
    i_gz1.append(q.copy(sx.at[0, :, h1], gz1.at[1], ZR))
    gx_send(5)
    q.landed(oz1.at[0], i_oz[0], ZR)
    op[2, :, qh0] = (op[2, :, qh0].astype(F32) + oz1[0].astype(F32)).astype(BF)
    i_oz.append(q.copy(op.at[2, :, qh0], oz2.at[0, :, qh0], ZL))
    q.landed(oz1.at[1], i_oz[1], ZL)
    op[1, :, qh1] = (op[1, :, qh1].astype(F32) + oz1[1].astype(F32)).astype(BF)
    i_oz.append(q.copy(op.at[1, :, qh1], oz2.at[1, :, qh1], ZR))
    gx_pass(3)
    gx_sum(2)
    i_gz2 = [q.copy(sx.at[1, :, h0], gz2.at[1, :, h0], ZR)]
    gx_send(6)
    gx_pass(4)
    gx_sum(3)
    i_gz2.append(q.copy(sx.at[2, :, h1], gz2.at[0, :, h1], ZL))
    gx_send(7)
    gx_pass(5)
    gx_pass(6)
    q.landed(gz1.at[1], i_gz1[1], ZL)
    gx_sum(4, (1,))
    i_gz2.append(q.copy(sx.at[1, :, h1], gz2.at[1, :, h1], ZR))
    gx_pass(7)

    q.landed(oz2.at[1, :, qh0], i_oz[2], ZL)
    q.landed(oz2.at[0, :, qh1], i_oz[3], ZR)
    q.landed(oz2.at[0, :, qh0], i_oz[4], ZR)
    q.landed(oz2.at[1, :, qh1], i_oz[5], ZL)

    def sum_out(k, _):
        rr = pl.ds(pl.multiple_of(k * rows, rows), rows)
        total = op[3, rr, :].astype(F32) + oz2[0, rr, :].astype(F32) + oz2[1, rr, :].astype(F32)
        fo[k] = total.astype(BF)
        return 0

    lax.fori_loop(0, 4, sum_out, 0)
    i_fa = [q.copy(fo.at[k], fa.at[a], peer) for peer, k in ((XR, aR), (XL, aL), (XO, aO))]
    fa[a] = fo[a]

    q.landed(gz1.at[0], i_gz1[0], ZR)
    gx_sum(5, (0,))
    i_gz2.append(q.copy(sx.at[2, :, h0], gz2.at[0, :, h0], ZL))

    f_sin.wait()
    gx_sum(6)
    gx_sum(7)

    for i, peer, src_a in zip(i_fa, (XL, XR, XO), (aL, aR, aO)):
        q.landed(fa.at[src_a], i, peer)
    for k in range(4):
        cols = slice(k * quarter, (k + 1) * quarter)
        fout[:, cols] = (inp[:, cols].astype(F32) + fa[k].astype(F32)).astype(BF)

    q.landed(ups, i_shift_b, SR)
    q.landed(gz2.at[1, :, h0], i_gz2[0], ZL)
    q.landed(gz2.at[0, :, h1], i_gz2[1], ZR)
    q.landed(gz2.at[1, :, h1], i_gz2[2], ZL)
    q.landed(gz2.at[0, :, h0], i_gz2[3], ZR)

    def back_rows(r, _):
        rr = pl.ds(pl.multiple_of(r * 16, 16), 16)
        total = sx[3, rr, :].astype(F32) + gz2[0, rr, :].astype(F32) + gz2[1, rr, :].astype(F32)
        lab = lt[1, pl.ds(pl.multiple_of(t * rows + r * 16, 16), 16), 0:1]
        scaled = total * jnp.where(lab == 0.0, gain[0:1, :], gain[1:2, :])
        x = sinv[rr, :].astype(F32)
        inv = lax.rsqrt(jnp.mean(x * x, axis=-1, keepdims=True) + EPSILON)
        corr = jnp.mean(scaled * x, axis=-1, keepdims=True)
        up = jnp.where(s == n_sec - 1, topv[rr, :], ups[rr, :]).astype(F32)
        bout[rr, :] = (up + inv * scaled - x * inv * inv * inv * corr).astype(BF)
        return 0

    lax.fori_loop(0, rows // 16, back_rows, 0)
    q.drain()


def body(
    embedded, previous_out, top_grad, grad_out, saved_input, saved_qkv, norm_gain, qkv_weight, out_weight,
    modality, documents,
):
    rows, width = embedded.shape
    length = saved_qkv.shape[1]
    blocks = length // rows
    quarter = width // 4
    wq = jnp.transpose(qkv_weight[0], (0, 2, 1, 3))
    sqkv = jnp.transpose(saved_qkv[0], (1, 0, 2))
    vm = pl.BlockSpec(memory_space=pltpu.VMEM)
    hb = pl.BlockSpec(memory_space=pltpu.HBM)
    v = pltpu.VMEM
    out = jax.ShapeDtypeStruct((rows, width), BF)
    chunk = 4 * rows
    def far(x):
        return pltpu.with_memory_space_constraint(x, pltpu.HBM)

    fwd, bwd = pl.pallas_call(
        kernel,
        out_shape=(out, out),
        in_specs=[hb] * 11,
        out_specs=(vm, vm),
        scratch_shapes=[
            v((2, width), F32),
            v((2, length), jnp.int32),
            v((2, length), jnp.int32),
            v((width, 768), BF),
            v((2, 4, 128, quarter), BF),
            v((rows, width), BF),
            v((rows, width), BF),
            v((rows, width), BF),
            v((rows, width), BF),
            v((rows, width), BF),
            v((3, length, HEAD_DIM), BF),
            v((blocks, rows, width), BF),
            v((length, 384), BF),
            v((4, length, HEAD_DIM), BF),
            v((4, chunk, quarter), BF),
            v((2, chunk, quarter // 2), BF),
            v((2, chunk, quarter), BF),
            v((4, rows, quarter), BF),
            v((4, rows, quarter), BF),
            v((4, chunk, quarter), BF),
            v((4, length, HEAD_DIM), BF),
            v((4, length, HEAD_DIM), BF),
            v((length, HEAD_DIM), BF),
            v((length, length), F32),
            v((length, length), BF),
            v((8, 128), F32),
            v((length, 768), BF),
            v((blocks, rows, width), BF),
            v((4, 2, rows, width // 2), BF),
            v((4, 2, rows, width), BF),
            v((4, rows, width), BF),
            v((2, rows, width // 2), BF),
            v((2, rows, width), BF),
            v((2, length, 128), F32),
            v((2, length, 128), F32),
            v((chunk, 768), F32),
            pltpu.SemaphoreType.DMA((N_SEMS,)),
            pltpu.SemaphoreType.DMA((N_SEMS,)),
            pltpu.SemaphoreType.DMA((N_LOCAL,)),
        ],
        compiler_params=pltpu.CompilerParams(
            collective_id=0, has_side_effects=True, vmem_limit_bytes=50 * 1024 * 1024
        ),
        name="relay",
    )(
        far(embedded), far(previous_out[0]), far(top_grad), far(grad_out[0]), far(saved_input[0]), far(sqkv),
        far(norm_gain[0]), far(wq), far(out_weight[0]), far(modality[0]), far(documents[0]),
    )
    return fwd[None], bwd[None]


def solution(mesh):
    placed = (
        P("tp", None),
        P("section", "tp", None),
        P("tp", None),
        P("section", "tp", None),
        P("section", "tp", None),
        P("section", None, None, "tp"),
        P("section", None, None),
        P("section", None, None, None, "tp"),
        P("section", None, "tp", None),
        P("section", None, None),
        P("section", None, None),
    )
    return jax.shard_map(
        body,
        mesh=mesh,
        in_specs=placed,
        out_specs=(P("section", "tp", None), P("section", "tp", None)),
        check_vma=False,
    )
```
